32 devices in a mesh: expert: 4 (over y, x), tensor: 4 (over z), rep: 2 (over core).
Axes of the slice: x: 2, y: 2, z: 4, core: 2. Of those that a mesh axis runs over, the one named last changes fastest.
Arguments:
- requests: bfloat16 [512, 1536], P('expert', ('tensor', 'rep')), may hold values from -6 to 6
- expert_ids: int32 [512, 2], P('expert'), may hold values from 0 to 3, all different within a row; in each aligned block of 128 rows (0 to 127, 128 to 255, ...) at most 96 rows name the same one
- gate_values: float32 [512, 2], P('expert'), may hold values from 0.2 to 1
- w_up: bfloat16 [4, 1536, 6144], P(None, 'expert', ('tensor', 'rep')), may hold values from -0.15625 to 0.15625
- w_down: bfloat16 [4, 1536, 6144], P(None, 'expert', ('tensor', 'rep')), may hold values from -0.078125 to 0.078125
- tower_in: bfloat16 [1536, 768], P(('tensor', 'rep')), may hold values from -0.15625 to 0.15625
- tower_bias: float32 [768], replicated, may hold values from -3 to 3
- tower_out: float32 [3, 256], replicated, may hold values from -0.375 to 0.375
- out_bias: float32 [3], replicated, may hold values from -3 to 3
Outputs:
- mixed: bfloat16 [512, 1536], P('expert', ('tensor', 'rep'))
- scores: float32 [3, 512], P(None, ('expert', 'tensor', 'rep'))
The draws below stay inside these ranges and needn't reach their ends.
Inputs may be any that keep to these rules, and one draw needn't show every extreme that they name: `expert_ids`: each row names two different experts. In the rows of one device (128 requests) no expert is named more than 96 times, a bound that some block reaches.
All inputs are finite; a program needn't handle non-finite values.
Results may differ from the reference program's by a relative error of at most 0.015.
Values may be sent and summed in bfloat16 or wider, within the bound.
A program may use at most 64 MiB of HBM per device.

```python
import math
import jax
import jax.numpy as jnp
import numpy as np
from jax import lax

D = 1536
HID = 6144
TH = 256
TASKS = 3
TOK_DEV = 128
EXPERTS = 4
CAP = 96
TOKENS = 512
N_TENSOR = 4
N_REP = 2


def block_scale(key, dims, shards, smallest, largest):
    def one(position, blocks):
        steps = jax.random.uniform(jax.random.fold_in(jax.random.fold_in(key, 6), position), (blocks,), jnp.float32, smallest / len(shards), largest / len(shards))
        return jnp.repeat(jnp.exp(steps), dims[position] // blocks).reshape((-1,) + (1,) * (len(dims) - position - 1))

    loudness = one(*shards[0])
    for cut in shards[1:]:
        loudness = loudness * one(*cut)
    return loudness


def assign_block(own_key, own, number, rows, number_of, top, bound, slope):
    order = jax.random.permutation(own_key, number_of)
    packed, common = shares(number_of, rows * top, bound, slope, True), shares(number_of, rows * top, bound, slope, False)
    places = jnp.arange(number_of)

    def named(sizes, turn):
        used = int((sizes > 0).sum())
        fixed = max(1, used // 4)
        moved = fixed + (places - fixed + turn * (used - fixed)) % max(1, number_of - fixed)
        return jnp.zeros((number_of,), jnp.int32).at[order[jnp.where(places < fixed, places, moved)]].set(jnp.asarray(sizes, jnp.int32))

    sizes = jnp.where(number % 4 == 0, named(packed, number // 4), named(common, number - number // 4 - 1))
    mixed = jax.random.permutation(jax.random.fold_in(own, 3), number_of)
    donor, receiver = mixed[0:number_of // 2 * 2:2], mixed[1:number_of // 2 * 2:2]
    room = jnp.minimum(sizes[donor] - 1, bound - sizes[receiver]) // 2
    room = jnp.where((donor == order[0]) | (receiver == order[0]) | (sizes[receiver] == 0), 0, jnp.maximum(room, 0))
    moved = jax.random.randint(jax.random.fold_in(own, 4), (number_of // 2,), 0, 1 << 20) % (room + 1)
    sizes = sizes.at[donor].add(-moved).at[receiver].add(moved)
    items = jnp.searchsorted(jnp.cumsum(sizes), jnp.arange(rows * top), side="right").astype(jnp.int32)
    table = items.reshape(top, rows).T
    table = table[jax.random.permutation(jax.random.fold_in(own, 1), rows)]
    turn = jax.random.randint(jax.random.fold_in(own, 2), (rows, 1), 0, top)
    return jnp.take_along_axis(table, (jnp.arange(top)[None, :] + turn) % top, axis=1)


def shares(number_of, total, most, slope, full):
    weights = [(1 << 20) // math.isqrt(standing ** slope) + 1 for standing in range(1, number_of + 1)]
    largest = most if full else min(most, max(-(-total // number_of), total * weights[0] // sum(weights)))
    least = 1 if total - largest >= number_of - 1 else 0
    holding, surplus = [largest] + [least] * (number_of - 1), total - largest - least * (number_of - 1)
    while surplus > 0:
        movable = [i for i in range(1, number_of) if holding[i] < largest] or [i for i in range(1, number_of) if holding[i] < most]
        mass, budget = sum([weights[i] for i in movable]), surplus
        for i in movable:
            extra = min(most - holding[i], max(1, budget * weights[i] // mass), surplus)
            holding[i] = holding[i] + extra
            surplus = surplus - extra
    return np.array(holding)


def normal_values(stream_key, extent, scale, reach, cuts=(), held_as=jnp.bfloat16):
    factor_of = block_scale(stream_key, extent, cuts, -0.22, 0.18) if cuts else 1.0
    values = jax.random.normal(stream_key, extent, jnp.float32) * scale * factor_of
    return jnp.minimum(jnp.maximum(values, -reach), reach).astype(held_as)


def setup_inputs(seed: int = 0) -> dict:
    key_list = jax.random.split(jax.random.key(seed), 10)
    requests = normal_values(key_list[0], (TOKENS, D), 1.0, 6.0, ((0, 4), (1, 8)))
    expert_ids_keys = jax.random.split(jax.random.fold_in(key_list[1], 1), TOKENS // TOK_DEV)
    expert_ids_turns = jax.random.permutation(jax.random.fold_in(key_list[1], 3), TOKENS // TOK_DEV)
    expert_ids = jax.vmap(lambda own, number: assign_block(jax.random.fold_in(key_list[1], 2), own, number, TOK_DEV, EXPERTS, 2, CAP, 2))(expert_ids_keys, expert_ids_turns).reshape((TOKENS, 2))
    gate_values = jnp.clip(0.2 + 0.8 * jax.random.uniform(key_list[2], (TOKENS, 2), jnp.float32) ** block_scale(key_list[2], (TOKENS, 2), ((0, 4),), -0.2, 0.2), 0.2, 1.0)
    w_up = normal_values(key_list[3], (EXPERTS, D, HID), D ** -0.5, 0.15625, ((1, 4), (2, 8)))
    w_down = normal_values(key_list[4], (EXPERTS, D, HID), HID ** -0.5, 0.078125, ((1, 4), (2, 8)))
    tower_in = normal_values(key_list[5], (D, TASKS * TH), D ** -0.5, 0.15625, ((0, 8),))
    tower_bias = normal_values(key_list[6], (TASKS * TH,), 0.5, 3.0, (), jnp.float32)
    tower_out = normal_values(key_list[7], (TASKS, TH), TH ** -0.5, 0.375, (), jnp.float32)
    out_bias = normal_values(key_list[8], (TASKS,), 1.0, 3.0, (), jnp.float32)
    return {"requests": requests, "expert_ids": expert_ids, "gate_values": gate_values, "w_up": w_up, "w_down": w_down, "tower_in": tower_in, "tower_bias": tower_bias, "tower_out": tower_out, "out_bias": out_bias}


def slot_table(expert_ids):
    blocks = expert_ids.reshape(-1, TOK_DEV * 2)
    onehot = (blocks[:, :, None] == jnp.arange(EXPERTS, dtype=jnp.int32)[None, None, :]).astype(jnp.int32)
    before = jnp.cumsum(onehot, axis=1) - onehot
    slot_rank = jnp.sum(before * onehot, axis=2)
    return (blocks * CAP + slot_rank).reshape(-1, 2)


def reference(requests, expert_ids, gate_values, w_up, w_down, tower_in, tower_bias, tower_out, out_bias):
    slots = slot_table(expert_ids)
    nblocks = TOKENS // TOK_DEV
    block_of = jnp.arange(TOKENS, dtype=jnp.int32) // TOK_DEV
    flat_index = (block_of[:, None] * (EXPERTS * CAP) + slots).astype(jnp.int32)
    dispatched = jnp.zeros((nblocks * EXPERTS * CAP, D), jnp.bfloat16)
    dispatched = dispatched.at[flat_index.reshape(-1)].set(jnp.repeat(requests, 2, axis=0))
    grouped = dispatched.reshape(nblocks, EXPERTS, CAP, D).transpose(1, 0, 2, 3).reshape(EXPERTS, nblocks * CAP, D)
    groups_hid = N_TENSOR * N_REP
    width = HID // groups_hid

    def expert_ffn(operands):
        rows, up_mat, down_mat = operands
        hidden = jax.nn.relu(jnp.dot(rows, up_mat, preferred_element_type=jnp.float32)).astype(jnp.bfloat16)
        total = jnp.zeros((rows.shape[0], D), jnp.float32)
        for group in range(groups_hid):
            part = jnp.dot(hidden[:, group * width:(group + 1) * width],
                           down_mat[:, group * width:(group + 1) * width].T,
                           preferred_element_type=jnp.float32)
            rounded = lax.optimization_barrier(part.astype(jnp.bfloat16))
            total = total + rounded.astype(jnp.float32)
        return total.astype(jnp.bfloat16)

    expert_out = lax.map(expert_ffn, (grouped, w_up, w_down))
    back = expert_out.reshape(EXPERTS, nblocks, CAP, D).transpose(1, 0, 2, 3).reshape(nblocks * EXPERTS * CAP, D)
    first = back[flat_index[:, 0]].astype(jnp.float32)
    second = back[flat_index[:, 1]].astype(jnp.float32)
    mixed = (gate_values[:, 0:1] * first + gate_values[:, 1:2] * second).astype(jnp.bfloat16)
    pre = jnp.dot(mixed, tower_in, preferred_element_type=jnp.float32) + tower_bias[None, :]
    active = jax.nn.relu(pre).reshape(TOKENS, TASKS, TH)
    logits = jnp.sum(active * tower_out[None, :, :], axis=2) + out_bias[None, :]
    scores = jax.nn.sigmoid(logits).T
    return mixed, scores
```

```python
import functools
import jax
import jax.numpy as jnp
from jax import lax
from jax.experimental import pallas as pl
from jax.experimental.pallas import tpu as pltpu
from jax.sharding import PartitionSpec as P

MESH = pl.DeviceIdType.MESH
CHUNKS = 2
F32 = jnp.float32
BF16 = jnp.bfloat16


def stay_kernel(
    dims, req_ref, meta_ref, up_hbm, down_hbm, tin_hbm, bias_ref, tout_ref, ob_ref,
    mixed_ref, scores_ref,
    up, down, tin, ag, meta, xin, xs, hp, r1, s2, r2, hid, mine, dsend0, drecv0, dsend, drecv,
    fsend, frecv, lsem, ag_s, ag_r, me_s, me_r, x_s, x_r, s1_s, s1_r, s2_s, s2_r, h_s, h_r,
    p_s, p_r, d_s, d_r, f_s, f_r,
):
    nx, nt, nr, experts, tok, feat, hcols, tasks, th = dims
    xe, t, r = lax.axis_index("expert"), lax.axis_index("tensor"), lax.axis_index("rep")
    sub = tok // CHUNKS
    started = []

    def remote(src, dst, ssem, rsem, dev):
        return pltpu.make_async_remote_copy(
            src_ref=src, dst_ref=dst, send_sem=ssem, recv_sem=rsem, device_id=dev,
            device_id_type=MESH)

    def send(src, dst, ssem, rsem, dev):
        copy = remote(src, dst, ssem, rsem, dev)
        copy.start()
        started.append((None, copy))

    def send_if(cond, src, dst, ssem, rsem, dev):
        copy = remote(src, dst, ssem, rsem, dev)

        @pl.when(cond)
        def _():
            copy.start()
        started.append((cond, copy))

    def got(ref, ssem, rsem):
        remote(ref, ref, ssem, rsem, (xe, t, r)).wait_recv()

    for d in range(1, nt):
        to = lax.rem(t + d, nt)
        send(req_ref, ag.at[t], ag_s.at[d], ag_r.at[t], (xe, to, r))
    for d in range(1, nx):
        send(meta_ref, meta.at[xe], me_s.at[d], me_r.at[xe], (xe ^ d, t, r))
    loads = [
        pltpu.make_async_copy(up_hbm, up, lsem.at[0]),
        pltpu.make_async_copy(down_hbm, down, lsem.at[1]),
        pltpu.make_async_copy(tin_hbm, tin, lsem.at[2]),
    ]
    for load in loads:
        load.start()
    meta[xe] = meta_ref[...]

    for d in (3, 1, 2, 0):
        tx = xe ^ d
        own = tx == t

        @pl.when(jnp.logical_not(own))
        def _():
            got(ag.at[tx], ag_s.at[0], ag_r.at[tx])
        for flip in (0, 1):
            if d == 0 and flip == 0:
                continue
            ss, rs = x_s.at[2 * d + flip], x_r.at[xe, r]
            dev = (tx, t, r ^ flip)
            send_if(own, req_ref, xin.at[xe, r], ss, rs, dev)
            send_if(jnp.logical_not(own), ag.at[tx], xin.at[xe, r], ss, rs, dev)

    is_own = xe == t

    @pl.when(is_own)
    def _():
        xin[xe, r] = req_ref[...]

    @pl.when(jnp.logical_not(is_own))
    def _():
        xin[xe, r] = ag[xe]

    for d in range(1, nx):
        got(meta.at[xe ^ d], me_s.at[0], me_r.at[xe ^ d])
    for d in range(nx):
        for flip in range(nr):
            if d == 0 and flip == 0:
                continue
            slot = (xe ^ d, r ^ flip)
            got(xin.at[slot], x_s.at[0], x_r.at[slot])
    for b in range(nx):
        for k in range(nr):
            xs[b, :, k * feat:(k + 1) * feat] = xin[b, k]
    info = [meta[b].T for b in range(nx)]

    def column(c, j):
        return jnp.concatenate([info[b][c * sub:(c + 1) * sub, j:j + 1] for b in range(nx)], axis=0)

    loads[0].wait()
    quarter = xe
    near = (1, 2)
    for c in range(CHUNKS):
        rows = xs[:, c * sub:(c + 1) * sub, :].reshape(nx * sub, nr * feat)
        ids = (column(c, 0), column(c, 1))
        for h in range(2):
            picked = [jnp.zeros((nx * sub, hcols), F32)] * 2
            for e in range(experts):
                part = jnp.dot(rows, up[e, :, h * hcols:(h + 1) * hcols], preferred_element_type=F32)
                picked = [jnp.where(ids[k] == float(e), part, picked[k]) for k in range(2)]
            for k in range(2):
                hp[c, h, :, k * sub:(k + 1) * sub, :] = picked[k].astype(BF16).reshape(nx, sub, hcols)
            fa, fb = near[h], near[1 - h]
            for i, q in enumerate((quarter ^ fa ^ fb, quarter ^ fa)):
                send(hp.at[c, h, q], r1.at[c, h, i], s1_s.at[c, h, i], s1_r.at[c, h, i],
                     (xe ^ fa, t, r))

    def reduce_first(c, h):
        fa, fb = near[h], near[1 - h]
        got(r1.at[c, h, 0], s1_s.at[c, h, 0], s1_r.at[c, h, 0])
        s2[c, h] = (hp[c, h, quarter ^ fb].astype(F32) + r1[c, h, 0].astype(F32)).astype(BF16)
        send(s2.at[c, h], r2.at[c, h], s2_s.at[c, h], s2_r.at[c, h], (xe ^ fb, t, r))

    def reduce_second(c, h):
        fa, fb = near[h], near[1 - h]
        got(r1.at[c, h, 1], s1_s.at[c, h, 1], s1_r.at[c, h, 1])
        got(r2.at[c, h], s2_s.at[c, h], s2_r.at[c, h])
        total = (hp[c, h, quarter].astype(F32) + r1[c, h, 1].astype(F32)) + r2[c, h].astype(F32)
        hid[c, h, quarter] = jnp.maximum(total, 0.0).astype(BF16)
        for i, f in enumerate((fb, fa)):
            send(hid.at[c, h, quarter], hid.at[c, h, quarter], h_s.at[c, h, i],
                 h_r.at[c, h, quarter], (xe ^ f, t, r))

    def forward(c, h):
        fa, fb = near[h], near[1 - h]
        q = quarter ^ fb
        got(hid.at[c, h, q], h_s.at[c, h, 2], h_r.at[c, h, q])
        send(hid.at[c, h, q], hid.at[c, h, q], h_s.at[c, h, 2], h_r.at[c, h, q], (xe ^ fa, t, r))

    def collect(c, h):
        fa, fb = near[h], near[1 - h]
        for q in (quarter ^ fa, quarter ^ fa ^ fb):
            got(hid.at[c, h, q], h_s.at[c, h, 2], h_r.at[c, h, q])

    def down_chunk(c):
        ids = (column(c, 0), column(c, 1))
        gates = (column(c, 2), column(c, 3))
        total = jnp.zeros((nx * sub, nr * feat), F32)
        for e in range(experts):
            hit = (ids[0] == float(e), ids[1] == float(e))
            weight = jnp.where(hit[0], gates[0], 0.0) + jnp.where(hit[1], gates[1], 0.0)
            part = None
            for h in range(2):
                values = [hid[c, h, :, k * sub:(k + 1) * sub, :].reshape(nx * sub, hcols)
                          for k in range(2)]
                chosen = jnp.where(hit[0], values[0], jnp.where(hit[1], values[1], jnp.zeros_like(values[1])))
                one = lax.dot_general(chosen, down[e, :, h * hcols:(h + 1) * hcols],
                                      (((1,), (1,)), ((), ())), preferred_element_type=F32)
                part = one if part is None else part + one
            total = total + weight * part
        low, high = total[:, :feat], total[:, feat:]
        mine[c] = jnp.where(r == 0, low, high).reshape(nx, sub, feat)
        dsend0[c] = jnp.where(r == 0, high, low).astype(BF16).reshape(nx, sub, feat)
        send(dsend0.at[c], drecv0.at[c], p_s.at[c], p_r.at[c], (xe, t, 1 - r))

    here = t == xe

    def pair_chunk(c):
        got(drecv0.at[c], p_s.at[c], p_r.at[c])
        dsend[c] = (mine[c] + drecv0[c].astype(F32)).astype(BF16)
        for b in range(nx):
            self_copy = jnp.logical_and(here, xe == b)

            @pl.when(self_copy)
            def _():
                drecv[c, t] = dsend[c, b]
            send_if(jnp.logical_not(self_copy), dsend.at[c, b], drecv.at[c, t], d_s.at[c, b],
                    d_r.at[c, t], (b, xe, r))

    def mixed_chunk(c):
        for src in range(nt):
            @pl.when(jnp.logical_not(jnp.logical_and(here, t == src)))
            def _():
                got(drecv.at[c, src], d_s.at[c, 0], d_r.at[c, src])
        total = drecv[c, 0].astype(F32)
        for src in range(1, nt):
            total = total + drecv[c, src].astype(F32)
        value = total.astype(BF16)
        mixed_ref[c * sub:(c + 1) * sub, :] = value
        part = jnp.dot(value, tin[...], preferred_element_type=F32).astype(BF16)
        each = tok // (nt * nr)
        per = sub // each
        fsend[c * per:(c + 1) * per] = part.reshape(per, each, part.shape[1])

    todo = [(c, h) for c in range(CHUNKS) for h in range(2)]
    for c in range(CHUNKS):
        for h in range(2):
            reduce_first(c, h)
        for h in range(2):
            reduce_second(c, h)
    loads[1].wait()
    loads[2].wait()
    for c in range(CHUNKS):
        for h in range(2):
            forward(c, h)
    for c in range(CHUNKS):
        for h in range(2):
            collect(c, h)
        down_chunk(c)
    for c in range(CHUNKS):
        pair_chunk(c)
    for c in range(CHUNKS):
        mixed_chunk(c)
    me = t * nr + r
    for d in range(1, nt * nr):
        to = me ^ d
        send(fsend.at[to], frecv.at[me], f_s.at[d], f_r.at[me],
             (xe, lax.div(to, nr), lax.rem(to, nr)))
    pre = fsend[me].astype(F32)
    for d in range(1, nt * nr):
        frm = me ^ d
        got(frecv.at[frm], f_s.at[d], f_r.at[frm])
        pre = pre + frecv[frm].astype(F32)
    active = jnp.maximum(pre + bias_ref[...], 0.0)
    outs = []
    for j in range(tasks):
        outs.append(jnp.sum(active[:, j * th:(j + 1) * th] * tout_ref[j:j + 1, :], axis=1, keepdims=True))
    each = pre.shape[0]
    lane = lax.broadcasted_iota(jnp.int32, (each, 128), 1)
    logits = jnp.zeros((each, 128), F32)
    for j in range(tasks):
        logits = jnp.where(lane == j, outs[j], logits)
    flipped = logits.T[:tasks, :] + ob_ref[...]
    scores_ref[...] = jax.nn.sigmoid(flipped)
    for cond, copy in started:
        if cond is None:
            copy.wait_send()
        else:
            @pl.when(cond)
            def _(copy=copy):
                copy.wait_send()


def stay_device(requests, expert_ids, gate_values, w_up, w_down, tower_in, tower_bias, tower_out,
                out_bias):
    nx, nt, nr = lax.axis_size("expert"), lax.axis_size("tensor"), lax.axis_size("rep")
    experts, _, hid_cols = w_up.shape
    tok, feat = requests.shape
    tasks, th = tower_out.shape
    hcols = hid_cols // 2
    sub = tok // CHUNKS
    each = tok // (nt * nr)
    dims = (nx, nt, nr, experts, tok, feat, hcols, tasks, th)
    meta = jnp.concatenate(
        [expert_ids.T.astype(F32), gate_values.T, jnp.zeros((4, tok), F32)], axis=0)
    vmem = pl.BlockSpec(memory_space=pltpu.VMEM)
    hbm = pl.BlockSpec(memory_space=pl.ANY)
    dma = pltpu.SemaphoreType.DMA
    C = CHUNKS
    scratch = [
        pltpu.VMEM(w_up.shape, BF16), pltpu.VMEM(w_down.shape, BF16),
        pltpu.VMEM(tower_in.shape, BF16),
        pltpu.VMEM((nt, tok, feat), BF16), pltpu.VMEM((nx, 8, tok), F32),
        pltpu.VMEM((nx, nr, tok, feat), BF16), pltpu.VMEM((nx, tok, nr * feat), BF16),
        pltpu.VMEM((C, 2, nx, 2 * sub, hcols), BF16),
        pltpu.VMEM((C, 2, 2, 2 * sub, hcols), BF16),
        pltpu.VMEM((C, 2, 2 * sub, hcols), BF16), pltpu.VMEM((C, 2, 2 * sub, hcols), BF16),
        pltpu.VMEM((C, 2, nx, 2 * sub, hcols), BF16),
        pltpu.VMEM((C, nx, sub, feat), F32), pltpu.VMEM((C, nx, sub, feat), BF16),
        pltpu.VMEM((C, nx, sub, feat), BF16), pltpu.VMEM((C, nx, sub, feat), BF16),
        pltpu.VMEM((C, nt, sub, feat), BF16),
        pltpu.VMEM((nt * nr, each, tasks * th), BF16), pltpu.VMEM((nt * nr, each, tasks * th), BF16),
        dma((3,)), dma((nt,)), dma((nt,)), dma((nx,)), dma((nx,)), dma((2 * nx,)), dma((nx, nr)),
        dma((C, 2, 2)), dma((C, 2, 2)), dma((C, 2)), dma((C, 2)), dma((C, 2, 3)), dma((C, 2, nx)),
        dma((C,)), dma((C,)), dma((C, nx)), dma((C, nt)), dma((nt * nr,)), dma((nt * nr,)),
    ]
    return pl.pallas_call(
        functools.partial(stay_kernel, dims),
        out_shape=(jax.ShapeDtypeStruct((tok, feat), BF16), jax.ShapeDtypeStruct((tasks, each), F32)),
        in_specs=[vmem, vmem, hbm, hbm, hbm, vmem, vmem, vmem],
        out_specs=(vmem, vmem),
        scratch_shapes=scratch,
        compiler_params=pltpu.CompilerParams(has_side_effects=True, vmem_limit_bytes=48 << 20),
        name="stay",
    )(requests, meta, w_up, w_down, tower_in, tower_bias[None, :], tower_out, out_bias[:, None])


def weights_stay(mesh):
    return mesh.shape["expert"] == 4 and mesh.shape["tensor"] == 4 and mesh.shape["rep"] == 2


def tower_head(pre, tower_bias, tower_out, out_bias):
    active = jax.nn.relu(pre + tower_bias[None, :])
    active = active.reshape(pre.shape[0], tower_out.shape[0], tower_out.shape[1])
    logits = jnp.sum(active * tower_out[None, :, :], axis=2) + out_bias[None, :]
    return jax.nn.sigmoid(logits).T


def per_device(
    requests, expert_ids, gate_values, w_up, w_down, tower_in, tower_bias, tower_out, out_bias
):
    groups = lax.axis_size("expert")
    experts = w_up.shape[0]
    local_experts = experts // groups
    tok_rows = requests.shape[0]
    capacity = 3 * tok_rows // experts
    serve_up, serve_down = (
        lax.all_to_all(w_up, "expert", split_axis=0, concat_axis=1, tiled=True),
        lax.all_to_all(w_down, "expert", split_axis=0, concat_axis=1, tiled=True),
    )
    flat_ids = expert_ids.reshape(-1)
    onehot = (flat_ids[:, None] == jnp.arange(experts, dtype=jnp.int32)[None, :]).astype(jnp.int32)
    before = jnp.cumsum(onehot, axis=0) - onehot
    slot_rank = jnp.sum(before * onehot, axis=1)
    slots = (flat_ids * capacity + slot_rank).reshape(tok_rows, 2)
    slot_index = jnp.arange(experts * capacity, dtype=jnp.int32)
    spread = (
        (slot_index[:, None] == slots[None, :, 0]) | (slot_index[:, None] == slots[None, :, 1])
    ).astype(jnp.bfloat16)
    full_rows = lax.all_gather(requests, ("tensor", "rep"), axis=1, tiled=True)
    outgoing = jnp.dot(spread, full_rows, preferred_element_type=jnp.float32).astype(jnp.bfloat16)
    incoming = lax.all_to_all(outgoing, "expert", split_axis=0, concat_axis=0, tiled=True)
    shaped = incoming.reshape(groups, local_experts, capacity, incoming.shape[1])
    hidden_pre = jnp.einsum("secd,edh->sech", shaped, serve_up, preferred_element_type=jnp.float32)
    hidden = jax.nn.relu(hidden_pre).astype(jnp.bfloat16)
    partial_value = jnp.einsum(
        "sech,edh->secd", hidden, serve_down, preferred_element_type=jnp.float32
    )
    summed = lax.psum_scatter(
        partial_value.astype(jnp.bfloat16), ("tensor", "rep"), scatter_dimension=3, tiled=True
    ).astype(jnp.float32)
    expert_out = summed.astype(jnp.bfloat16).reshape(
        groups * local_experts * capacity, summed.shape[3]
    )
    returned = lax.all_to_all(expert_out, "expert", split_axis=0, concat_axis=0, tiled=True)
    pick_first = (slots[:, 0:1] == slot_index[None, :]).astype(jnp.bfloat16)
    pick_second = (slots[:, 1:2] == slot_index[None, :]).astype(jnp.bfloat16)
    first = jnp.dot(pick_first, returned, preferred_element_type=jnp.float32)
    second = jnp.dot(pick_second, returned, preferred_element_type=jnp.float32)
    mixed = (gate_values[:, 0:1] * first + gate_values[:, 1:2] * second).astype(jnp.bfloat16)
    pre = lax.psum_scatter(
        jnp.dot(mixed, tower_in, preferred_element_type=jnp.float32).astype(jnp.bfloat16),
        ("tensor", "rep"),
        scatter_dimension=0,
        tiled=True,
    ).astype(jnp.float32)
    scores = tower_head(pre, tower_bias, tower_out, out_bias)
    return (mixed, scores)


def solution(mesh):
    in_specs = (
        P("expert", ("tensor", "rep")),
        P("expert", None),
        P("expert", None),
        P(None, "expert", ("tensor", "rep")),
        P(None, "expert", ("tensor", "rep")),
        P(("tensor", "rep"), None),
        P(),
        P(),
        P(),
    )
    out_specs = (P("expert", ("tensor", "rep")), P(None, ("expert", "tensor", "rep")))
    body = stay_device if weights_stay(mesh) else per_device
    return jax.shard_map(
        body, mesh=mesh, in_specs=in_specs, out_specs=out_specs, check_vma=False
    )
```

```python
import functools
import jax
import jax.numpy as jnp
from jax import lax
from jax.experimental import pallas as pl
from jax.experimental.pallas import tpu as pltpu
from jax.sharding import PartitionSpec as P

MESH = pl.DeviceIdType.MESH
CHUNKS = 4
F32 = jnp.float32
BF16 = jnp.bfloat16


def stay_kernel(
    dims, req_hbm, ids_hbm, gates_hbm, up_hbm, down_hbm, tin_hbm, bias_hbm, tout_hbm, ob_ref,
    mixed_ref, scores_ref,
    req_ref, ids_ref, gates_ref, bias_ref, tout_ref, up, down, tin, ag, meta_ref, meta, xin, xs, hp, r1, s2, r2, hid, mine, dsend0, drecv0, dsend, drecv,
    fsend, frecv, mixed_rows, lsem, ag_s, ag_r, me_s, me_r, x_s, x_r, s1_s, s1_r, s2_s, s2_r, h_s, h_r,
    p_s, p_r, d_s, d_r, f_s, f_r,
):
    nx, nt, nr, experts, tok, feat, hcols, tasks, th = dims
    xe, t, r = lax.axis_index("expert"), lax.axis_index("tensor"), lax.axis_index("rep")
    sub = tok // CHUNKS
    started = []

    def remote(src, dst, ssem, rsem, dev):
        return pltpu.make_async_remote_copy(
            src_ref=src, dst_ref=dst, send_sem=ssem, recv_sem=rsem, device_id=dev,
            device_id_type=MESH)

    def send(src, dst, ssem, rsem, dev):
        copy = remote(src, dst, ssem, rsem, dev)
        copy.start()
        started.append((None, copy))

    def send_if(cond, src, dst, ssem, rsem, dev):
        copy = remote(src, dst, ssem, rsem, dev)

        @pl.when(cond)
        def _():
            copy.start()
        started.append((cond, copy))

    def got(ref, ssem, rsem):
        remote(ref, ref, ssem, rsem, (xe, t, r)).wait_recv()

    first = [
        pltpu.make_async_copy(req_hbm, req_ref, lsem.at[3]),
        pltpu.make_async_copy(ids_hbm, ids_ref, lsem.at[4]),
        pltpu.make_async_copy(gates_hbm, gates_ref, lsem.at[5]),
    ]
    loads = [
        pltpu.make_async_copy(up_hbm, up, lsem.at[0]),
        pltpu.make_async_copy(down_hbm, down, lsem.at[1]),
        pltpu.make_async_copy(tin_hbm, tin, lsem.at[2]),
        pltpu.make_async_copy(bias_hbm, bias_ref, lsem.at[6]),
        pltpu.make_async_copy(tout_hbm, tout_ref, lsem.at[7]),
    ]
    for load in first + loads:
        load.start()
    here = t == xe
    barrier = pltpu.get_barrier_semaphore()

    def greet(dev):
        pl.semaphore_signal(barrier, inc=1, device_id=dev, device_id_type=MESH)

    me = t * nr + r
    for d in range(1, nt * nr):
        other = me ^ d
        greet((xe, lax.div(other, nr), lax.rem(other, nr)))
    for d in range(1, nx):
        for flip in range(nr):
            greet((xe ^ d, t, r ^ flip))
    for b in range(nx):
        @pl.when(jnp.logical_not(jnp.logical_and(here, xe == b)))
        def _():
            greet((b, xe, r))

        @pl.when(jnp.logical_not(jnp.logical_and(here, t == b)))
        def _():
            greet((t, b, r))
    for load in first:
        load.wait()
    meta_ref[...] = jnp.concatenate(
        [ids_ref[...].astype(F32), gates_ref[...], jnp.zeros((4, tok), F32)], axis=0)
    greeted = (nt * nr - 1) + (nx - 1) * nr + 2 * nx

    @pl.when(here)
    def _():
        pl.semaphore_wait(barrier, greeted - 2)

    @pl.when(jnp.logical_not(here))
    def _():
        pl.semaphore_wait(barrier, greeted)

    for d in range(1, nt):
        to = lax.rem(t + d, nt)
        send(req_ref, ag.at[t], ag_s.at[d], ag_r.at[t], (xe, to, r))
    for d in range(1, nx):
        send(meta_ref, meta.at[xe], me_s.at[d], me_r.at[xe], (xe ^ d, t, r))
    meta[xe] = meta_ref[...]

    for d in (3, 1, 2, 0):
        tx = xe ^ d
        own = tx == t

        @pl.when(jnp.logical_not(own))
        def _():
            got(ag.at[tx], ag_s.at[0], ag_r.at[tx])
        for flip in (0, 1):
            if d == 0 and flip == 0:
                continue
            ss, rs = x_s.at[2 * d + flip], x_r.at[xe, r]
            dev = (tx, t, r ^ flip)
            send_if(own, req_ref, xin.at[xe, r], ss, rs, dev)
            send_if(jnp.logical_not(own), ag.at[tx], xin.at[xe, r], ss, rs, dev)

    is_own = xe == t

    @pl.when(is_own)
    def _():
        xin[xe, r] = req_ref[...]

    @pl.when(jnp.logical_not(is_own))
    def _():
        xin[xe, r] = ag[xe]

    for d in range(1, nx):
        got(meta.at[xe ^ d], me_s.at[0], me_r.at[xe ^ d])
    for d in range(nx):
        for flip in range(nr):
            if d == 0 and flip == 0:
                continue
            slot = (xe ^ d, r ^ flip)
            got(xin.at[slot], x_s.at[0], x_r.at[slot])
    for b in range(nx):
        for k in range(nr):
            xs[b, :, k * feat:(k + 1) * feat] = xin[b, k].T
    info = [meta[b].T for b in range(nx)]

    def column(c, j):
        return jnp.concatenate([info[b][c * sub:(c + 1) * sub, j:j + 1] for b in range(nx)], axis=0)

    loads[0].wait()
    quarter = xe
    near = (1, 2)
    def up_chunk(c):
        rows = xs[:, c * sub:(c + 1) * sub, :].reshape(nx * sub, nr * feat)
        ids = (column(c, 0), column(c, 1))
        for h in range(2):
            picked = [jnp.zeros((nx * sub, hcols), F32)] * 2
            for e in range(experts):
                part = jnp.dot(rows, up[e, :, h * hcols:(h + 1) * hcols], preferred_element_type=F32)
                picked = [jnp.where(ids[k] == float(e), part, picked[k]) for k in range(2)]
            for k in range(2):
                hp[c, h, :, k * sub:(k + 1) * sub, :] = picked[k].astype(BF16).reshape(nx, sub, hcols)
            fa, fb = near[h], near[1 - h]
            for i, q in enumerate((quarter ^ fa ^ fb, quarter ^ fa)):
                send(hp.at[c, h, q], r1.at[c, h, i], s1_s.at[c, h, i], s1_r.at[c, h, i],
                     (xe ^ fa, t, r))

    def reduce_first(c, h):
        fa, fb = near[h], near[1 - h]
        got(r1.at[c, h, 0], s1_s.at[c, h, 0], s1_r.at[c, h, 0])
        s2[c, h] = (hp[c, h, quarter ^ fb].astype(F32) + r1[c, h, 0].astype(F32)).astype(BF16)
        send(s2.at[c, h], r2.at[c, h], s2_s.at[c, h], s2_r.at[c, h], (xe ^ fb, t, r))

    def reduce_second(c, h):
        fa, fb = near[h], near[1 - h]
        got(r1.at[c, h, 1], s1_s.at[c, h, 1], s1_r.at[c, h, 1])
        got(r2.at[c, h], s2_s.at[c, h], s2_r.at[c, h])
        total = (hp[c, h, quarter].astype(F32) + r1[c, h, 1].astype(F32)) + r2[c, h].astype(F32)
        hid[c, h, quarter] = jnp.maximum(total, 0.0).astype(BF16)
        for i, f in enumerate((fb, fa)):
            send(hid.at[c, h, quarter], hid.at[c, h, quarter], h_s.at[c, h, i],
                 h_r.at[c, h, quarter], (xe ^ f, t, r))

    def forward(c, h):
        fa, fb = near[h], near[1 - h]
        q = quarter ^ fb
        got(hid.at[c, h, q], h_s.at[c, h, 2], h_r.at[c, h, q])
        send(hid.at[c, h, q], hid.at[c, h, q], h_s.at[c, h, 2], h_r.at[c, h, q], (xe ^ fa, t, r))

    def collect(c, h):
        fa, fb = near[h], near[1 - h]
        for q in (quarter ^ fa, quarter ^ fa ^ fb):
            got(hid.at[c, h, q], h_s.at[c, h, 2], h_r.at[c, h, q])

    def down_chunk(c):
        ids = (column(c, 0), column(c, 1))
        gates = (column(c, 2), column(c, 3))
        total = jnp.zeros((nx * sub, nr * feat), F32)
        for e in range(experts):
            hit = (ids[0] == float(e), ids[1] == float(e))
            weight = jnp.where(hit[0], gates[0], 0.0) + jnp.where(hit[1], gates[1], 0.0)
            part = None
            for h in range(2):
                values = [hid[c, h, :, k * sub:(k + 1) * sub, :].reshape(nx * sub, hcols)
                          for k in range(2)]
                chosen = jnp.where(hit[0], values[0], jnp.where(hit[1], values[1], jnp.zeros_like(values[1])))
                one = lax.dot_general(chosen, down[e, :, h * hcols:(h + 1) * hcols],
                                      (((1,), (1,)), ((), ())), preferred_element_type=F32)
                part = one if part is None else part + one
            total = total + weight * part
        low, high = total[:, :feat], total[:, feat:]
        mine[c] = jnp.where(r == 0, low, high).reshape(nx, sub, feat)
        dsend0[c] = jnp.where(r == 0, high, low).astype(BF16).reshape(nx, sub, feat)
        send(dsend0.at[c], drecv0.at[c], p_s.at[c], p_r.at[c], (xe, t, 1 - r))

    def pair_chunk(c):
        got(drecv0.at[c], p_s.at[c], p_r.at[c])
        dsend[c] = (mine[c] + drecv0[c].astype(F32)).astype(BF16)
        for b in range(nx):
            self_copy = jnp.logical_and(here, xe == b)

            @pl.when(self_copy)
            def _():
                drecv[c, t] = dsend[c, b]
            send_if(jnp.logical_not(self_copy), dsend.at[c, b], drecv.at[c, t], d_s.at[c, b],
                    d_r.at[c, t], (b, xe, r))

    def mixed_chunk(c):
        for src in range(nt):
            @pl.when(jnp.logical_not(jnp.logical_and(here, t == src)))
            def _():
                got(drecv.at[c, src], d_s.at[c, 0], d_r.at[c, src])
        total = drecv[c, 0].astype(F32)
        for src in range(1, nt):
            total = total + drecv[c, src].astype(F32)
        value = total.astype(BF16)
        mixed_rows[c * sub:(c + 1) * sub, :] = value
        part = jnp.dot(value, tin[...], preferred_element_type=F32).astype(BF16)
        each = tok // (nt * nr)
        per = sub // each
        fsend[c * per:(c + 1) * per] = part.reshape(per, each, part.shape[1])
        for to in range(c * per, (c + 1) * per):
            send_if(me != to, fsend.at[to], frecv.at[me], f_s.at[to], f_r.at[me],
                    (xe, to // nr, to % nr))

    def both(stage, c):
        if 0 <= c < CHUNKS:
            for h in range(2):
                stage(c, h)

    def one(stage, c):
        if 0 <= c < CHUNKS:
            stage(c)

    for i in range(CHUNKS + 8):
        if i == 5:
            for load in loads[1:]:
                load.wait()
        both(forward, i - 4)
        both(reduce_second, i - 3)
        both(reduce_first, i - 2)
        one(up_chunk, i)
        both(collect, i - 5)
        one(down_chunk, i - 5)
        one(pair_chunk, i - 6)
        one(mixed_chunk, i - 7)
    mixed_ref[...] = mixed_rows[...].T
    pre = fsend[me].astype(F32)
    for d in range(1, nt * nr):
        frm = me ^ d
        got(frecv.at[frm], f_s.at[0], f_r.at[frm])
        pre = pre + frecv[frm].astype(F32)
    active = jnp.maximum(pre + bias_ref[...].reshape(1, tasks * th), 0.0)
    outs = []
    for j in range(tasks):
        outs.append(jnp.sum(active[:, j * th:(j + 1) * th] * tout_ref[j:j + 1, :], axis=1, keepdims=True))
    each = pre.shape[0]
    lane = lax.broadcasted_iota(jnp.int32, (each, 128), 1)
    logits = jnp.zeros((each, 128), F32)
    for j in range(tasks):
        logits = jnp.where(lane == j, outs[j] + ob_ref[j], logits)
    scores_ref[...] = jax.nn.sigmoid(logits.T[:tasks, :])
    for cond, copy in started:
        if cond is None:
            copy.wait_send()
        else:
            @pl.when(cond)
            def _(copy=copy):
                copy.wait_send()


def stay_device(requests, expert_ids, gate_values, w_up, w_down, tower_in, tower_bias, tower_out,
                out_bias):
    nx, nt, nr = lax.axis_size("expert"), lax.axis_size("tensor"), lax.axis_size("rep")
    experts, _, hid_cols = w_up.shape
    tok, feat = requests.shape
    tasks, th = tower_out.shape
    hcols = hid_cols // 2
    sub = tok // CHUNKS
    each = tok // (nt * nr)
    dims = (nx, nt, nr, experts, tok, feat, hcols, tasks, th)
    vmem = pl.BlockSpec(memory_space=pltpu.VMEM)
    hbm = pl.BlockSpec(memory_space=pltpu.HBM)
    smem = pl.BlockSpec(memory_space=pltpu.SMEM)
    dma = pltpu.SemaphoreType.DMA
    C = CHUNKS
    scratch = [
        pltpu.VMEM((feat, tok), BF16), pltpu.VMEM((2, tok), jnp.int32), pltpu.VMEM((2, tok), F32),
        pltpu.VMEM(tower_bias.shape, F32), pltpu.VMEM(tower_out.shape, F32),
        pltpu.VMEM(w_up.shape, BF16), pltpu.VMEM(w_down.shape, BF16),
        pltpu.VMEM(tower_in.shape, BF16),
        pltpu.VMEM((nt, feat, tok), BF16), pltpu.VMEM((8, tok), F32), pltpu.VMEM((nx, 8, tok), F32),
        pltpu.VMEM((nx, nr, feat, tok), BF16), pltpu.VMEM((nx, tok, nr * feat), BF16),
        pltpu.VMEM((C, 2, nx, 2 * sub, hcols), BF16),
        pltpu.VMEM((C, 2, 2, 2 * sub, hcols), BF16),
        pltpu.VMEM((C, 2, 2 * sub, hcols), BF16), pltpu.VMEM((C, 2, 2 * sub, hcols), BF16),
        pltpu.VMEM((C, 2, nx, 2 * sub, hcols), BF16),
        pltpu.VMEM((C, nx, sub, feat), F32), pltpu.VMEM((C, nx, sub, feat), BF16),
        pltpu.VMEM((C, nx, sub, feat), BF16), pltpu.VMEM((C, nx, sub, feat), BF16),
        pltpu.VMEM((C, nt, sub, feat), BF16),
        pltpu.VMEM((nt * nr, each, tasks * th), BF16), pltpu.VMEM((nt * nr, each, tasks * th), BF16),
        pltpu.VMEM((tok, feat), BF16),
        dma((8,)), dma((nt,)), dma((nt,)), dma((nx,)), dma((nx,)), dma((2 * nx,)), dma((nx, nr)),
        dma((C, 2, 2)), dma((C, 2, 2)), dma((C, 2)), dma((C, 2)), dma((C, 2, 3)), dma((C, 2, nx)),
        dma((C,)), dma((C,)), dma((C, nx)), dma((C, nt)), dma((nt * nr,)), dma((nt * nr,)),
    ]
    mixed, scores = pl.pallas_call(
        functools.partial(stay_kernel, dims),
        out_shape=(jax.ShapeDtypeStruct((feat, tok), BF16), jax.ShapeDtypeStruct((tasks, each), F32)),
        in_specs=[hbm] * 8 + [smem],
        out_specs=(vmem, vmem),
        scratch_shapes=scratch,
        compiler_params=pltpu.CompilerParams(
            has_side_effects=True, collective_id=0, vmem_limit_bytes=60 << 20),
        name="stay",
    )(requests.T, expert_ids.T, gate_values.T, w_up, w_down, tower_in, tower_bias, tower_out, out_bias)
    return mixed.T, scores


def weights_stay(mesh):
    return mesh.shape["expert"] == 4 and mesh.shape["tensor"] == 4 and mesh.shape["rep"] == 2


def tower_head(pre, tower_bias, tower_out, out_bias):
    active = jax.nn.relu(pre + tower_bias[None, :])
    active = active.reshape(pre.shape[0], tower_out.shape[0], tower_out.shape[1])
    logits = jnp.sum(active * tower_out[None, :, :], axis=2) + out_bias[None, :]
    return jax.nn.sigmoid(logits).T


def per_device(
    requests, expert_ids, gate_values, w_up, w_down, tower_in, tower_bias, tower_out, out_bias
):
    groups = lax.axis_size("expert")
    experts = w_up.shape[0]
    local_experts = experts // groups
    tok_rows = requests.shape[0]
    capacity = 3 * tok_rows // experts
    serve_up, serve_down = (
        lax.all_to_all(w_up, "expert", split_axis=0, concat_axis=1, tiled=True),
        lax.all_to_all(w_down, "expert", split_axis=0, concat_axis=1, tiled=True),
    )
    flat_ids = expert_ids.reshape(-1)
    onehot = (flat_ids[:, None] == jnp.arange(experts, dtype=jnp.int32)[None, :]).astype(jnp.int32)
    before = jnp.cumsum(onehot, axis=0) - onehot
    slot_rank = jnp.sum(before * onehot, axis=1)
    slots = (flat_ids * capacity + slot_rank).reshape(tok_rows, 2)
    slot_index = jnp.arange(experts * capacity, dtype=jnp.int32)
    spread = (
        (slot_index[:, None] == slots[None, :, 0]) | (slot_index[:, None] == slots[None, :, 1])
    ).astype(jnp.bfloat16)
    full_rows = lax.all_gather(requests, ("tensor", "rep"), axis=1, tiled=True)
    outgoing = jnp.dot(spread, full_rows, preferred_element_type=jnp.float32).astype(jnp.bfloat16)
    incoming = lax.all_to_all(outgoing, "expert", split_axis=0, concat_axis=0, tiled=True)
    shaped = incoming.reshape(groups, local_experts, capacity, incoming.shape[1])
    hidden_pre = jnp.einsum("secd,edh->sech", shaped, serve_up, preferred_element_type=jnp.float32)
    hidden = jax.nn.relu(hidden_pre).astype(jnp.bfloat16)
    partial_value = jnp.einsum(
        "sech,edh->secd", hidden, serve_down, preferred_element_type=jnp.float32
    )
    summed = lax.psum_scatter(
        partial_value.astype(jnp.bfloat16), ("tensor", "rep"), scatter_dimension=3, tiled=True
    ).astype(jnp.float32)
    expert_out = summed.astype(jnp.bfloat16).reshape(
        groups * local_experts * capacity, summed.shape[3]
    )
    returned = lax.all_to_all(expert_out, "expert", split_axis=0, concat_axis=0, tiled=True)
    pick_first = (slots[:, 0:1] == slot_index[None, :]).astype(jnp.bfloat16)
    pick_second = (slots[:, 1:2] == slot_index[None, :]).astype(jnp.bfloat16)
    first = jnp.dot(pick_first, returned, preferred_element_type=jnp.float32)
    second = jnp.dot(pick_second, returned, preferred_element_type=jnp.float32)
    mixed = (gate_values[:, 0:1] * first + gate_values[:, 1:2] * second).astype(jnp.bfloat16)
    pre = lax.psum_scatter(
        jnp.dot(mixed, tower_in, preferred_element_type=jnp.float32).astype(jnp.bfloat16),
        ("tensor", "rep"),
        scatter_dimension=0,
        tiled=True,
    ).astype(jnp.float32)
    scores = tower_head(pre, tower_bias, tower_out, out_bias)
    return (mixed, scores)


def solution(mesh):
    in_specs = (
        P("expert", ("tensor", "rep")),
        P("expert", None),
        P("expert", None),
        P(None, "expert", ("tensor", "rep")),
        P(None, "expert", ("tensor", "rep")),
        P(("tensor", "rep"), None),
        P(),
        P(),
        P(),
    )
    out_specs = (P("expert", ("tensor", "rep")), P(None, ("expert", "tensor", "rep")))
    body = stay_device if weights_stay(mesh) else per_device
    return jax.shard_map(
        body, mesh=mesh, in_specs=in_specs, out_specs=out_specs, check_vma=False
    )
```
